256 devices in a mesh: ctx: 32 (over y, z), head: 8 (over x, core).
Axes of the slice: x: 4, y: 4, z: 8, core: 2. Of those that a mesh axis runs over, the one named last changes fastest.
Arguments:
- queries: bfloat16 [65536, 8192], P('ctx', 'head'), may hold values from -9 to 9
- keys: bfloat16 [65536, 1024], P('ctx', 'head'), may hold values from -8 to 8
- values: bfloat16 [65536, 1024], P('ctx', 'head'), may hold values from -6 to 6
- source_block: int32 [512], replicated, may hold values from 0 to 511, as said below
- doc_of_block: int32 [512], replicated, may hold values from 0 to 112, never falling along the last dimension, each value on 1 to 8 neighbouring positions
Outputs:
- attended: bfloat16 [65536, 8192], P(('ctx', 'head'))
The draws below stay inside these ranges and needn't reach their ends.
Inputs may be any that keep to these rules, and one draw needn't show every extreme that they name: `source_block`: each number once. Generation row block b belongs to generation owner b // 16; pack block p lies on context shard p // 16; a context shard receives at most 1 block from one generation owner. `doc_of_block`: never falling along the pack; a rollout covers 1 to 8 blocks.
All inputs are finite; a program needn't handle non-finite values.
Results may differ from the reference program's by a relative error of at most 0.008.
Values may be sent and summed in bfloat16 or wider, within the bound.
No kernel may reach another device: no remote copies, remote signals or barrier semaphores. Data moves between devices by JAX's collectives and lax.ppermute only.
A program may use at most 64 MiB of HBM per device.

```python
import math
import jax
import jax.numpy as jnp
import numpy as np
from jax import lax

QUERY_HEADS = 64
KEY_VALUE_HEADS = 8
HEAD_SIZE = 128
TOK_DEV = 2048
BLK = 128
DOCMAX = 8
PACK_TOKENS = 65536
NB = 512
DOCS = 113
N_CTX = 32


def newest_values(key, shape):
    return jnp.clip(jax.random.normal(key, shape, jnp.float32), -6.0, 6.0)


def draw_queries(key, part):
    fresh_keys = newest_values(jax.random.fold_in(key, 1), (PACK_TOKENS, QUERY_HEADS * HEAD_SIZE))
    return fresh_keys.astype(jnp.bfloat16)


def draw_keys(key, part):
    fresh_keys = newest_values(jax.random.fold_in(key, 2), (PACK_TOKENS, KEY_VALUE_HEADS * HEAD_SIZE))
    return fresh_keys.astype(jnp.bfloat16)


def draw_source_block(key, part):
    per_shard = TOK_DEV // BLK
    shards = N_CTX
    capacity = max(1, per_shard // shards)
    pair_count = per_shard // capacity
    offset_key, label_key, slot_key, order_key = jax.random.split(key, 4)
    offsets = jax.random.permutation(offset_key, shards)[:pair_count]
    relabel = jax.random.permutation(label_key, shards)
    slot_scores = jax.random.randint(slot_key, (shards, per_shard), 0, 1024) * per_shard + jnp.arange(per_shard)[None, :]
    slot_perm = jnp.argsort(slot_scores, axis=1, stable=True)
    pair_index = slot_perm // capacity
    shard_ids = jnp.arange(shards)[:, None]
    owner_of = jnp.take(relabel, (shard_ids + jnp.take(offsets, pair_index)) % shards).reshape(-1)
    order_keys = jax.random.permutation(order_key, NB)
    same_owner = owner_of[:, None] == owner_of[None, :]
    before = order_keys[None, :] < order_keys[:, None]
    local_of = jnp.sum(same_owner & before, axis=1)
    return (owner_of * per_shard + local_of).astype(jnp.int32)


def steps_of(rng, extent, cuts, least, high):
    factor_of = 1.0
    for dim, blocks in cuts:
        heights = jax.random.uniform(jax.random.fold_in(jax.random.fold_in(rng, 6), dim), (blocks,), jnp.float32, least / len(cuts), high / len(cuts))
        factor_of = factor_of * jnp.repeat(jnp.exp(heights), extent[dim] // blocks).reshape((-1,) + (1,) * (len(extent) - 1 - dim))
    return factor_of


def profile(amount, total, bound, slope):
    loads = [(1 << 20) // math.isqrt(standing ** slope) + 1 for standing in range(2, amount + 1)]
    surplus, counts = total - bound - (amount - 1), [1] * (amount - 1)
    while surplus > 0:
        movable = [i for i in range(amount - 1) if counts[i] < bound]
        mass, left = sum([loads[i] for i in movable]), surplus
        for i in movable:
            extra = min(bound - counts[i], max(1, left * loads[i] // mass), surplus)
            counts[i] = counts[i] + extra
            surplus = surplus - extra
    return np.array([bound] + counts)


def uneven(own_key, number_of, total, limit, lean):
    if number_of == 2:
        one = jax.random.randint(own_key, (), max(1, total - limit), min(limit, total - 1) + 1)
        return jnp.stack([one, total - one])
    lengths = jnp.asarray(profile(number_of, total, limit, lean), jnp.int32)
    pairs = (number_of - 1) // 2
    donor, taker = lengths[1:1 + 2 * pairs:2], lengths[2:2 + 2 * pairs:2]
    room = jnp.minimum(donor - 1, limit - taker)
    shifted = jax.random.randint(jax.random.fold_in(own_key, 1), (pairs,), 0, 1 << 20) % (room + 1)
    lengths = lengths.at[1:1 + 2 * pairs:2].set(donor - shifted).at[2:2 + 2 * pairs:2].set(taker + shifted)
    return lengths[jax.random.permutation(jax.random.fold_in(own_key, 2), number_of)]


def centred(rng, shape, scale, bound, cuts=(), kind=jnp.bfloat16):
    values = scale * jax.random.normal(rng, shape, jnp.float32)
    if cuts:
        values = values * steps_of(rng, shape, cuts, -0.22, 0.18)
    return jnp.clip(values, -bound, bound).astype(kind)


def setup_inputs(seed: int = 0) -> dict:
    key_of = jax.random.split(jax.random.key(seed), 6)
    return {
        "queries": draw_queries(jax.random.fold_in(key_of[5], 71), 0),
        "keys": draw_keys(jax.random.fold_in(key_of[5], 71), 0),
        "values": centred(key_of[2], (PACK_TOKENS, KEY_VALUE_HEADS * HEAD_SIZE), 1.0, 6.0, ((0, 32), (1, 8))),
        "source_block": draw_source_block(jax.random.fold_in(key_of[5], 71), 0),
        "doc_of_block": jnp.searchsorted(jnp.cumsum(uneven(key_of[4], DOCS, NB, DOCMAX, 2)), jnp.arange(NB), side="right").astype(jnp.int32),
    }


def attend(query_block, key_window, value_window, window_docs):
    window = DOCMAX * BLK
    key_pos = jnp.arange(window)
    query_pos = (DOCMAX - 1) * BLK + jnp.arange(BLK)
    causal = key_pos[None, :] <= query_pos[:, None]
    same_doc = window_docs == window_docs[DOCMAX - 1]
    allowed = causal & same_doc[key_pos // BLK][None, :]
    scores = jnp.einsum("qngd,knd->ngqk", query_block.astype(jnp.float32), key_window.astype(jnp.float32)) * (HEAD_SIZE ** -0.5)
    masked = jnp.where(allowed, scores, -1e30)
    row_max = jnp.max(masked, axis=-1, keepdims=True)
    expo_terms = jnp.where(allowed, jnp.exp(masked - row_max), 0.0)
    weights = (expo_terms / jnp.sum(expo_terms, axis=-1, keepdims=True)).astype(jnp.bfloat16)
    mixed_out = jnp.einsum("ngqk,knd->qngd", weights.astype(jnp.float32), value_window.astype(jnp.float32))
    return mixed_out.astype(jnp.bfloat16)


def reference(queries, keys, values, source_block, doc_of_block):
    query_group_size = QUERY_HEADS // KEY_VALUE_HEADS

    def repacked_tokens(array):
        blocks = array.reshape(NB, BLK, array.shape[1])
        return jnp.take(blocks, source_block.astype(jnp.int32), axis=0).reshape(PACK_TOKENS, array.shape[1])

    packed_queries = repacked_tokens(queries).reshape(PACK_TOKENS, KEY_VALUE_HEADS, query_group_size, HEAD_SIZE)
    packed_keys = repacked_tokens(keys).reshape(PACK_TOKENS, KEY_VALUE_HEADS, HEAD_SIZE)
    packed_values = repacked_tokens(values).reshape(PACK_TOKENS, KEY_VALUE_HEADS, HEAD_SIZE)
    reachable_rows = (DOCMAX - 1) * BLK
    key_extended = jnp.concatenate([jnp.zeros((reachable_rows, KEY_VALUE_HEADS, HEAD_SIZE), packed_keys.dtype), packed_keys], axis=0)
    value_extended = jnp.concatenate([jnp.zeros((reachable_rows, KEY_VALUE_HEADS, HEAD_SIZE), packed_values.dtype), packed_values], axis=0)
    doc_ext = jnp.concatenate([jnp.full((DOCMAX - 1,), -1, jnp.int32), doc_of_block.astype(jnp.int32)])

    def one_block(block_index):
        row_start = block_index * BLK
        query_block = lax.dynamic_slice_in_dim(packed_queries, row_start, BLK, 0)
        key_window = lax.dynamic_slice_in_dim(key_extended, row_start, DOCMAX * BLK, 0)
        value_window = lax.dynamic_slice_in_dim(value_extended, row_start, DOCMAX * BLK, 0)
        window_docs = lax.dynamic_slice_in_dim(doc_ext, block_index, DOCMAX, 0)
        return attend(query_block, key_window, value_window, window_docs)

    stacked = lax.map(one_block, jnp.arange(NB, dtype=jnp.int32))
    return stacked.reshape(PACK_TOKENS, QUERY_HEADS * HEAD_SIZE)
```

```python
import functools
import math

import jax
import jax.numpy as jnp
from jax import lax
from jax.experimental import pallas as pl
from jax.experimental.pallas import tpu as pltpu
from jax.sharding import PartitionSpec as P


HEAD_SIZE = 128
BLK = 128
DOCMAX = 8
REACH = DOCMAX - 1
ROWS = (64, 48, 16)
TILE = 256
SCALE = HEAD_SIZE**-0.5 * math.log2(math.e)

SMEM = pl.BlockSpec(memory_space=pltpu.SMEM)
VMEM = pl.BlockSpec(memory_space=pltpu.VMEM)
HBM = pl.BlockSpec(memory_space=pl.ANY)


def pack_kv_out(dest, keys, values, out):
    def one(b, carry):
        s = dest[b]
        out[s, :, :HEAD_SIZE] = keys[b]
        out[s, :, HEAD_SIZE:] = values[b]
        return carry

    lax.fori_loop(0, keys.shape[0], one, 0)


def pack_queries(dest, queries, *outs):
    row = 0
    for out in outs:
        rows = out.shape[1]
        out[0] = queries[0, row : row + rows]
        row += rows


def pack_kv_in(owner, got, out):
    def one(b, carry):
        out[b] = got[owner[b]]
        return carry

    lax.fori_loop(0, out.shape[0], one, 0)


def attend(row0, spread, owner, count, seat, got, packed, halo, *refs):
    rows, width = got.shape[1], got.shape[2]
    heads = width // HEAD_SIZE
    blocks = packed.shape[0]
    if spread:
        outs, (out, key_scr, value_scr, sems) = refs[:-4], refs[-4:]
        pair = outs[0].shape[0]
    else:
        out, key_scr, value_scr = refs
    edge = REACH * BLK
    total = blocks * BLK
    key_scr[:edge] = halo[:, :, :HEAD_SIZE].reshape(edge, HEAD_SIZE)
    key_scr[edge:] = packed[:, :, :HEAD_SIZE].reshape(total, HEAD_SIZE)
    value_scr[:edge, :HEAD_SIZE] = halo[:, :, HEAD_SIZE:].reshape(edge, HEAD_SIZE)
    value_scr[edge:, :HEAD_SIZE] = packed[:, :, HEAD_SIZE:].reshape(total, HEAD_SIZE)
    value_scr[:, HEAD_SIZE:] = jnp.ones((edge + total, HEAD_SIZE), value_scr.dtype)
    step = max(d for d in range(1, heads + 1) if heads % d == 0 and d * rows <= TILE)
    row_of = row0 + lax.broadcasted_iota(jnp.int32, (step * rows, BLK), 0) % rows
    allowed = lax.broadcasted_iota(jnp.int32, (step * rows, BLK), 1) <= row_of

    def one(b, carry):
        slot = owner[b]
        if spread:
            at = ((b // pair) ^ seat[0]) * pair + b % pair
        else:
            at = b

        def with_blocks(n):
            start = pl.multiple_of((b + DOCMAX - n) * BLK, BLK)
            k = key_scr[pl.ds(start, n * BLK), :]
            v = value_scr[pl.ds(start, n * BLK), :]
            for first in range(0, heads, step):
                stacked = jnp.concatenate(
                    [
                        got[slot, :, h * HEAD_SIZE : (h + 1) * HEAD_SIZE]
                        for h in range(first, first + step)
                    ],
                    axis=0,
                )
                s = lax.dot_general(
                    stacked, k, (((1,), (1,)), ((), ())), preferred_element_type=jnp.float32
                )
                last = jnp.where(allowed, s[:, (n - 1) * BLK :], -1e30)
                s = last if n == 1 else jnp.concatenate([s[:, : (n - 1) * BLK], last], axis=1)
                m = jnp.max(s, axis=1, keepdims=True)
                p = jnp.exp2((s - m) * SCALE).astype(jnp.bfloat16)
                mixed = jnp.dot(p, v, preferred_element_type=jnp.float32)
                mixed = (mixed[:, :HEAD_SIZE] / mixed[:, HEAD_SIZE:]).astype(jnp.bfloat16)
                for h in range(step):
                    out[at, :, (first + h) * HEAD_SIZE : (first + h + 1) * HEAD_SIZE] = mixed[
                        h * rows : (h + 1) * rows
                    ]

        for n in range(1, DOCMAX + 1):
            pl.when(count[b] == n)(functools.partial(with_blocks, n))
        return carry

    lax.fori_loop(0, blocks, one, 0)
    if spread:
        copies = [
            pltpu.make_async_copy(out.at[pl.ds(k * pair, pair)], outs[k], sems.at[k])
            for k in range(len(outs))
        ]
        for copy in copies:
            copy.start()
        for copy in copies:
            copy.wait()


def place(row0, spread, chained, seat, *refs):
    out, sems = refs[-2], refs[-1]
    parts = refs[: -3 if chained else -2]
    groups = len(parts) if spread else parts[0].shape[0]
    copies = []
    for g in range(groups):
        part = parts[g] if spread else parts[0].at[g]
        h = g ^ seat[0] if spread else g
        pair, rows, width = part.shape
        for i in range(pair):
            copies.append(
                pltpu.make_async_copy(
                    part.at[i],
                    out.at[
                        pl.ds(i * BLK + row0, rows), pl.ds(pl.multiple_of(h * width, width), width)
                    ],
                    sems.at[g, i],
                )
            )
    for copy in copies:
        copy.start()
    for copy in copies:
        copy.wait()


def exchange(queries, keys, values, source_block, doc_of_block):
    shards = lax.axis_size("ctx")
    groups = lax.axis_size("head")
    me = lax.axis_index("ctx")
    seat = lax.axis_index("head").reshape(1)
    row_count, width = queries.shape
    blocks = row_count // BLK
    pair = blocks // groups
    dtype = queries.dtype
    pack_position = jnp.arange(shards * blocks, dtype=jnp.int32)
    held = me * blocks + jnp.arange(blocks, dtype=jnp.int32)
    position = jnp.sum(
        jnp.where(source_block[None, :] == held[:, None], pack_position[None, :], 0), axis=1
    )
    dest = position // blocks

    kv_out = pl.pallas_call(
        pack_kv_out,
        out_shape=jax.ShapeDtypeStruct((shards, BLK, 2 * HEAD_SIZE), dtype),
        in_specs=[SMEM, VMEM, VMEM],
        out_specs=VMEM,
        name="pack_kv_out",
    )(dest, keys.reshape(blocks, BLK, HEAD_SIZE), values.reshape(blocks, BLK, HEAD_SIZE))
    kv_got = lax.all_to_all(kv_out, "ctx", split_axis=0, concat_axis=0, tiled=True)

    q_out = pl.pallas_call(
        pack_queries,
        out_shape=[jax.ShapeDtypeStruct((shards, rows, width), dtype) for rows in ROWS],
        grid_spec=pltpu.PrefetchScalarGridSpec(
            num_scalar_prefetch=1,
            grid=(blocks,),
            in_specs=[pl.BlockSpec((1, BLK, width), lambda b, dest: (b, 0, 0))],
            out_specs=[
                pl.BlockSpec((1, rows, width), lambda b, dest: (dest[b], 0, 0)) for rows in ROWS
            ],
        ),
        name="pack_queries",
    )(dest, queries.reshape(blocks, BLK, width))
    q_got = []
    for q in q_out:
        q_got.append(lax.all_to_all(q, "ctx", split_axis=0, concat_axis=0, tiled=True))

    owner = lax.dynamic_slice_in_dim(source_block, me * blocks, blocks) // blocks
    doc_ext = jnp.concatenate([jnp.full((REACH,), -1, jnp.int32), doc_of_block])
    docs = lax.dynamic_slice_in_dim(doc_ext, me * blocks, blocks + REACH)
    count = sum(
        (docs[REACH - d : REACH - d + blocks] == docs[REACH:]).astype(jnp.int32)
        for d in range(DOCMAX)
    )

    packed = pl.pallas_call(
        pack_kv_in,
        out_shape=jax.ShapeDtypeStruct((blocks, BLK, 2 * HEAD_SIZE), dtype),
        in_specs=[SMEM, VMEM],
        out_specs=VMEM,
        name="pack_kv_in",
    )(owner, kv_got)
    route = [(i, i + 1) for i in range(shards - 1)]
    halo = lax.ppermute(packed[blocks - REACH :], "ctx", route)

    result = None
    row0 = 0
    scratch = [
        pltpu.VMEM(((blocks + REACH) * BLK, HEAD_SIZE), dtype),
        pltpu.VMEM(((blocks + REACH) * BLK, 2 * HEAD_SIZE), dtype),
    ]
    for r, (q, rows) in enumerate(zip(q_got, ROWS)):
        spread = r < len(ROWS) - 1
        if spread:
            shape = [jax.ShapeDtypeStruct((pair, rows, width), dtype)] * groups
            held_out = [pltpu.VMEM((blocks, rows, width), dtype)]
            sems = [pltpu.SemaphoreType.DMA((groups,))]
        else:
            shape = jax.ShapeDtypeStruct((blocks, rows, width), dtype)
            held_out = sems = []
        attended = pl.pallas_call(
            functools.partial(attend, row0, spread),
            out_shape=shape,
            in_specs=[SMEM, SMEM, SMEM, VMEM, VMEM, VMEM],
            out_specs=[HBM] * groups if spread else VMEM,
            scratch_shapes=held_out + scratch + sems,
        )(owner, count, seat, q, packed, halo)
        if spread:
            parts = [attended[0]]
            for k in range(1, groups):
                swap = [(i, i ^ k) for i in range(groups)]
                parts.append(lax.ppermute(attended[k], "head", swap))
        else:
            parts = [
                lax.all_to_all(
                    attended.reshape(groups, pair * rows, width),
                    "head",
                    split_axis=0,
                    concat_axis=0,
                    tiled=True,
                ).reshape(groups, pair, rows, width)
            ]
        before = [] if result is None else [result]
        result = pl.pallas_call(
            functools.partial(place, row0, spread, bool(before)),
            out_shape=jax.ShapeDtypeStruct((pair * BLK, groups * width), dtype),
            in_specs=[SMEM] + [VMEM] * len(parts) + [HBM] * len(before),
            out_specs=HBM,
            scratch_shapes=[pltpu.SemaphoreType.DMA((groups, pair))],
            input_output_aliases={1 + len(parts): 0} if before else {},
        )(seat, *parts, *before)
        row0 += rows
    return result


def solution(mesh):
    in_specs = (P("ctx", "head"), P("ctx", "head"), P("ctx", "head"), P(), P())
    out_specs = P(("ctx", "head"), None)
    return jax.shard_map(exchange, mesh=mesh, in_specs=in_specs, out_specs=out_specs, check_vma=False)
```

```python
import functools
import math

import jax
import jax.numpy as jnp
from jax import lax
from jax.experimental import pallas as pl
from jax.experimental.pallas import tpu as pltpu
from jax.sharding import PartitionSpec as P


HEAD_SIZE = 128
BLK = 128
DOCMAX = 8
REACH = DOCMAX - 1
ROWS = (96, 32)
GROUP = (1, 4)
HALVES = 1
COUNTS = (1, 2, 4, 6, 8)
TILE = 384
SCALE = HEAD_SIZE**-0.5 * math.log2(math.e)

SMEM = pl.BlockSpec(memory_space=pltpu.SMEM)
VMEM = pl.BlockSpec(memory_space=pltpu.VMEM)
HBM = pl.BlockSpec(memory_space=pl.ANY)


def pack_kv_out(dest, keys, values, out):
    def one(b, carry):
        s = dest[b]
        out[s, :, :HEAD_SIZE] = keys[b]
        out[s, :, HEAD_SIZE:] = values[b]
        return carry

    lax.fori_loop(0, keys.shape[0], one, 0)


def pack_queries(dest, queries, *outs):
    for r, out in enumerate(outs):
        row = sum(ROWS[:r])
        out[0] = queries[0, row : row + out.shape[1]]


def pack_kv_in(owner, got, out, sems):
    blocks = out.shape[0]
    copies = [
        pltpu.make_async_copy(got.at[owner[b]], out.at[b], sems.at[b]) for b in range(blocks)
    ]
    for copy in copies:
        copy.start()
    for copy in copies:
        copy.wait()


def attend(row0, group, first_seat, spot, owner, count, turn, got, packed, halo, *refs):
    spread = first_seat is not None
    queries, key_scr, value_scr, q_sems = refs[-4:]
    if spread:
        outs, (out, o_sems) = refs[:-6], refs[-6:-4]
        pair = outs[0].shape[0]
    else:
        out = refs[0]
    items, rows, width = out.shape
    blocks = packed.shape[0]
    heads = width // HEAD_SIZE

    def block_at(i):
        if spread:
            return ((first_seat + i // pair) ^ spot[1]) * pair + i % pair
        return turn[i]

    loads = [
        pltpu.make_async_copy(got.at[owner[block_at(i)]], queries.at[i], q_sems.at[i])
        for i in range(items)
    ]
    for load in loads:
        load.start()
    edge = REACH * BLK
    total = blocks * BLK
    key_scr[:edge] = halo[:, :, :HEAD_SIZE].reshape(edge, HEAD_SIZE)
    key_scr[edge:] = packed[:, :, :HEAD_SIZE].reshape(total, HEAD_SIZE)
    value_scr[:edge, :HEAD_SIZE] = halo[:, :, HEAD_SIZE:].reshape(edge, HEAD_SIZE)
    value_scr[edge:, :HEAD_SIZE] = packed[:, :, HEAD_SIZE:].reshape(total, HEAD_SIZE)
    value_scr[:, HEAD_SIZE:] = jnp.ones((edge + total, HEAD_SIZE), value_scr.dtype)
    step = max(d for d in range(1, heads + 1) if heads % d == 0 and d * rows <= TILE)
    row_of = row0 + lax.broadcasted_iota(jnp.int32, (step * rows, BLK), 0) % rows
    allowed = lax.broadcasted_iota(jnp.int32, (step * rows, BLK), 1) <= row_of
    for load in loads:
        load.wait()

    def some(i, carry):
        held = [(i * group + g, block_at(i * group + g)) for g in range(group)]
        most = count[held[0][1]]
        for _, b in held[1:]:
            most = jnp.maximum(most, count[b])

        def with_blocks(n):
            work = []
            for item, b in held:
                start = pl.multiple_of((b + DOCMAX - n) * BLK, BLK)
                k = key_scr[pl.ds(start, n * BLK), :]
                for first in range(0, heads, step):
                    stacked = jnp.concatenate(
                        [
                            queries[item, :, h * HEAD_SIZE : (h + 1) * HEAD_SIZE]
                            for h in range(first, first + step)
                        ],
                        axis=0,
                    )
                    s = lax.dot_general(
                        stacked, k, (((1,), (1,)), ((), ())), preferred_element_type=jnp.float32
                    )
                    work.append((item if spread else b, b, start, first, s))
            weighted = []
            for _, b, start, first, s in work:
                parts = [
                    s[:, j * BLK : (j + 1) * BLK] + jnp.where(n - j <= count[b], 0.0, -1e30)
                    for j in range(n - 1)
                ]
                parts.append(jnp.where(allowed, s[:, (n - 1) * BLK :], -1e30))
                m = functools.reduce(jnp.maximum, parts)
                m = jnp.max(m, axis=1, keepdims=True)
                p = [jnp.exp2((part - m) * SCALE).astype(jnp.bfloat16) for part in parts]
                p = p[0] if n == 1 else jnp.concatenate(p, axis=1)
                weighted.append(p)
            for (at, _, start, first, _), p in zip(work, weighted):
                v = value_scr[pl.ds(start, n * BLK), :]
                mixed = jnp.dot(p, v, preferred_element_type=jnp.float32)
                mixed = (mixed[:, :HEAD_SIZE] / mixed[:, HEAD_SIZE:]).astype(jnp.bfloat16)
                for h in range(step):
                    out[at, :, (first + h) * HEAD_SIZE : (first + h + 1) * HEAD_SIZE] = mixed[
                        h * rows : (h + 1) * rows
                    ]

        low = 0
        for n in COUNTS:
            pl.when((most > low) & (most <= n))(functools.partial(with_blocks, n))
            low = n
        return carry

    lax.fori_loop(0, items // group, some, 0)
    if spread:
        copies = [
            pltpu.make_async_copy(out.at[pl.ds(k * pair, pair)], outs[k], o_sems.at[k])
            for k in range(len(outs))
        ]
        for copy in copies:
            copy.start()
        for copy in copies:
            copy.wait()


def place(row0, spread, chained, spot, *refs):
    out, sems = refs[-2], refs[-1]
    parts = refs[: -3 if chained else -2]
    groups = len(parts) if spread else parts[0].shape[0]
    copies = []
    for g in range(groups):
        part = parts[g] if spread else parts[0].at[g]
        h = g ^ spot[1] if spread else g
        pair, rows, width = part.shape
        for i in range(pair):
            copies.append(
                pltpu.make_async_copy(
                    part.at[i],
                    out.at[
                        pl.ds(i * BLK + row0, rows), pl.ds(pl.multiple_of(h * width, width), width)
                    ],
                    sems.at[g, i],
                )
            )
    for copy in copies:
        copy.start()
    for copy in copies:
        copy.wait()


def exchange(queries, keys, values, source_block, doc_of_block):
    shards = lax.axis_size("ctx")
    groups = lax.axis_size("head")
    me = lax.axis_index("ctx")
    spot = jnp.stack([me, lax.axis_index("head")])
    row_count, width = queries.shape
    blocks = row_count // BLK
    pair = blocks // groups
    dtype = queries.dtype
    pack_position = jnp.arange(shards * blocks, dtype=jnp.int32)
    held = me * blocks + jnp.arange(blocks, dtype=jnp.int32)
    position = jnp.sum(
        jnp.where(source_block[None, :] == held[:, None], pack_position[None, :], 0), axis=1
    )
    dest = position // blocks

    kv_out = pl.pallas_call(
        pack_kv_out,
        out_shape=jax.ShapeDtypeStruct((shards, BLK, 2 * HEAD_SIZE), dtype),
        in_specs=[SMEM, VMEM, VMEM],
        out_specs=VMEM,
        name="pack_kv_out",
    )(dest, keys.reshape(blocks, BLK, HEAD_SIZE), values.reshape(blocks, BLK, HEAD_SIZE))
    kv_got = lax.all_to_all(kv_out, "ctx", split_axis=0, concat_axis=0, tiled=True)

    query_blocks = queries.reshape(blocks, BLK, width)
    q_out = pl.pallas_call(
        pack_queries,
        out_shape=[jax.ShapeDtypeStruct((shards, rows, width), dtype) for rows in ROWS],
        grid_spec=pltpu.PrefetchScalarGridSpec(
            num_scalar_prefetch=1,
            grid=(blocks,),
            in_specs=[pl.BlockSpec((1, BLK, width), lambda b, dest: (b, 0, 0))],
            out_specs=[
                pl.BlockSpec((1, rows, width), lambda b, dest: (dest[b], 0, 0)) for rows in ROWS
            ],
        ),
        name="pack_queries",
    )(dest, query_blocks)
    q_got = []
    for q in q_out:
        q_got.append(lax.all_to_all(q, "ctx", split_axis=0, concat_axis=0, tiled=True))

    owner = lax.dynamic_slice_in_dim(source_block, me * blocks, blocks) // blocks
    doc_ext = jnp.concatenate([jnp.full((REACH,), -1, jnp.int32), doc_of_block])
    docs = lax.dynamic_slice_in_dim(doc_ext, me * blocks, blocks + REACH)
    count = sum(
        (docs[REACH - d : REACH - d + blocks] == docs[REACH:]).astype(jnp.int32)
        for d in range(DOCMAX)
    )
    at = jnp.arange(blocks, dtype=jnp.int32)
    key = count * blocks + at
    rank = jnp.sum((key[None, :] < key[:, None]).astype(jnp.int32), axis=1)
    turn = jnp.sum(jnp.where(rank[None, :] == at[:, None], at[None, :], 0), axis=1)

    packed = pl.pallas_call(
        pack_kv_in,
        out_shape=jax.ShapeDtypeStruct((blocks, BLK, 2 * HEAD_SIZE), dtype),
        in_specs=[SMEM, HBM],
        out_specs=VMEM,
        scratch_shapes=[pltpu.SemaphoreType.DMA((blocks,))],
        name="pack_kv_in",
    )(owner, kv_got)
    route = [(i, i + 1) for i in range(shards - 1)]
    halo = lax.ppermute(packed[blocks - REACH :], "ctx", route)

    result = None
    row0 = 0
    for r, (got, rows) in enumerate(zip(q_got, ROWS)):
        spread = r < len(ROWS) - 1
        step = groups // HALVES if spread else groups
        parts = [None] * groups
        for first in reversed(range(0, groups, step)):
            items = step * pair
            scratch = [
                pltpu.VMEM((items, rows, width), dtype),
                pltpu.VMEM(((blocks + REACH) * BLK, HEAD_SIZE), dtype),
                pltpu.VMEM(((blocks + REACH) * BLK, 2 * HEAD_SIZE), dtype),
                pltpu.SemaphoreType.DMA((items,)),
            ]
            if spread:
                shape = [jax.ShapeDtypeStruct((pair, rows, width), dtype)] * step
                scratch = [
                    pltpu.VMEM((items, rows, width), dtype),
                    pltpu.SemaphoreType.DMA((step,)),
                ] + scratch
            else:
                shape = jax.ShapeDtypeStruct((blocks, rows, width), dtype)
            attended = pl.pallas_call(
                functools.partial(attend, row0, GROUP[r], first if spread else None),
                out_shape=shape,
                in_specs=[SMEM] * 4 + [HBM, VMEM, VMEM],
                out_specs=[HBM] * step if spread else VMEM,
                scratch_shapes=scratch,
            )(spot, owner, count, turn, got, packed, halo)
            if spread:
                for k in range(first, first + step):
                    swap = [(i, i ^ k) for i in range(groups)]
                    part = attended[k - first]
                    parts[k] = lax.ppermute(part, "head", swap) if k else part
            else:
                parts = [
                    lax.all_to_all(
                        attended.reshape(groups, pair * rows, width),
                        "head",
                        split_axis=0,
                        concat_axis=0,
                        tiled=True,
                    ).reshape(groups, pair, rows, width)
                ]
        before = [] if result is None else [result]
        result = pl.pallas_call(
            functools.partial(place, row0, spread, bool(before)),
            out_shape=jax.ShapeDtypeStruct((pair * BLK, groups * width), dtype),
            in_specs=[SMEM] + [VMEM] * len(parts) + [HBM] * len(before),
            out_specs=HBM,
            scratch_shapes=[pltpu.SemaphoreType.DMA((groups, pair))],
            input_output_aliases={1 + len(parts): 0} if before else {},
        )(spot, *parts, *before)
        row0 += rows
    return result


def solution(mesh):
    in_specs = (P("ctx", "head"), P("ctx", "head"), P("ctx", "head"), P(), P())
    out_specs = P(("ctx", "head"), None)
    return jax.shard_map(exchange, mesh=mesh, in_specs=in_specs, out_specs=out_specs, check_vma=False)
```

```python
import functools
import math

import jax
import jax.numpy as jnp
from jax import lax
from jax.experimental import pallas as pl
from jax.experimental.pallas import tpu as pltpu
from jax.sharding import PartitionSpec as P


HEAD_SIZE = 128
BLK = 128
DOCMAX = 8
REACH = DOCMAX - 1
ROWS = (96, 32)
GROUP = (2, 4)
HALVES = 1
COUNTS = (1, 2, 4, 6, 8)
TILE = 384
SCALE = HEAD_SIZE**-0.5 * math.log2(math.e)

SMEM = pl.BlockSpec(memory_space=pltpu.SMEM)
VMEM = pl.BlockSpec(memory_space=pltpu.VMEM)
HBM = pl.BlockSpec(memory_space=pl.ANY)


def pack_kv_out(dest, keys, values, out, sems):
    copies = []
    for b in range(keys.shape[0]):
        for i, array in enumerate((keys, values)):
            columns = pl.ds(i * HEAD_SIZE, HEAD_SIZE)
            copies.append(
                pltpu.make_async_copy(array.at[b], out.at[dest[b], :, columns], sems.at[i, b])
            )
    for copy in copies:
        copy.start()
    for copy in copies:
        copy.wait()


def pack_queries(dest, queries, *outs):
    for r, out in enumerate(outs):
        row = sum(ROWS[:r])
        out[0] = queries[0, row : row + out.shape[1]]


def pack_kv_in(owner, got, out, sems):
    blocks = out.shape[0]
    copies = [
        pltpu.make_async_copy(got.at[owner[b]], out.at[b], sems.at[b]) for b in range(blocks)
    ]
    for copy in copies:
        copy.start()
    for copy in copies:
        copy.wait()


def attend(row0, group, first_seat, spot, owner, count, turn, got, packed, halo, *refs):
    spread = first_seat is not None
    queries, key_scr, value_scr, q_sems = refs[-4:]
    if spread:
        outs, (out, o_sems) = refs[:-6], refs[-6:-4]
        pair = outs[0].shape[0]
    else:
        out = refs[0]
    items, rows, width = out.shape
    blocks = packed.shape[0]
    heads = width // HEAD_SIZE

    def block_at(i):
        if spread:
            return ((first_seat + i // pair) ^ spot[1]) * pair + i % pair
        return turn[i]

    loads = [
        pltpu.make_async_copy(got.at[owner[block_at(i)]], queries.at[i], q_sems.at[i])
        for i in range(items)
    ]
    for load in loads:
        load.start()
    edge = REACH * BLK
    total = blocks * BLK
    key_scr[:edge] = halo[:, :, :HEAD_SIZE].reshape(edge, HEAD_SIZE)
    key_scr[edge:] = packed[:, :, :HEAD_SIZE].reshape(total, HEAD_SIZE)
    value_scr[:edge, :HEAD_SIZE] = halo[:, :, HEAD_SIZE:].reshape(edge, HEAD_SIZE)
    value_scr[edge:, :HEAD_SIZE] = packed[:, :, HEAD_SIZE:].reshape(total, HEAD_SIZE)
    value_scr[:, HEAD_SIZE:] = jnp.ones((edge + total, HEAD_SIZE), value_scr.dtype)
    step = max(d for d in range(1, heads + 1) if heads % d == 0 and d * rows <= TILE)
    row_of = row0 + lax.broadcasted_iota(jnp.int32, (step * rows, BLK), 0) % rows
    allowed = lax.broadcasted_iota(jnp.int32, (step * rows, BLK), 1) <= row_of
    if spread:
        for load in loads:
            load.wait()

    def some(i, carry):
        if not spread:
            for g in range(group):
                at = i * group + g
                pltpu.make_async_copy(
                    got.at[owner[block_at(at)]], queries.at[at], q_sems.at[at]
                ).wait()
        held = [(i * group + g, block_at(i * group + g)) for g in range(group)]
        most = count[held[0][1]]
        for _, b in held[1:]:
            most = jnp.maximum(most, count[b])

        def with_blocks(n):
            work = []
            for item, b in held:
                start = pl.multiple_of((b + DOCMAX - n) * BLK, BLK)
                k = key_scr[pl.ds(start, n * BLK), :]
                for first in range(0, heads, step):
                    stacked = jnp.concatenate(
                        [
                            queries[item, :, h * HEAD_SIZE : (h + 1) * HEAD_SIZE]
                            for h in range(first, first + step)
                        ],
                        axis=0,
                    )
                    s = lax.dot_general(
                        stacked, k, (((1,), (1,)), ((), ())), preferred_element_type=jnp.float32
                    )
                    work.append((item if spread else b, b, start, first, s))
            weighted = []
            for _, b, start, first, s in work:
                parts = [
                    s[:, j * BLK : (j + 1) * BLK] + jnp.where(n - j <= count[b], 0.0, -1e30)
                    for j in range(n - 1)
                ]
                parts.append(jnp.where(allowed, s[:, (n - 1) * BLK :], -1e30))
                m = functools.reduce(jnp.maximum, parts)
                m = jnp.max(m, axis=1, keepdims=True)
                p = [jnp.exp2((part - m) * SCALE).astype(jnp.bfloat16) for part in parts]
                p = p[0] if n == 1 else jnp.concatenate(p, axis=1)
                weighted.append(p)
            for (at, _, start, first, _), p in zip(work, weighted):
                v = value_scr[pl.ds(start, n * BLK), :]
                mixed = jnp.dot(p, v, preferred_element_type=jnp.float32)
                mixed = (mixed[:, :HEAD_SIZE] / mixed[:, HEAD_SIZE:]).astype(jnp.bfloat16)
                for h in range(step):
                    out[at, :, (first + h) * HEAD_SIZE : (first + h + 1) * HEAD_SIZE] = mixed[
                        h * rows : (h + 1) * rows
                    ]

        low = 0
        for n in COUNTS:
            pl.when((most > low) & (most <= n))(functools.partial(with_blocks, n))
            low = n
        return carry

    lax.fori_loop(0, items // group, some, 0)
    if spread:
        copies = [
            pltpu.make_async_copy(out.at[pl.ds(k * pair, pair)], outs[k], o_sems.at[k])
            for k in range(len(outs))
        ]
        for copy in copies:
            copy.start()
        for copy in copies:
            copy.wait()


def place(row0, spread, chained, spot, *refs):
    out, sems = refs[-2], refs[-1]
    parts = refs[: -3 if chained else -2]
    groups = len(parts) if spread else parts[0].shape[0]
    copies = []
    for g in range(groups):
        part = parts[g] if spread else parts[0].at[g]
        h = g ^ spot[1] if spread else g
        pair, rows, width = part.shape
        for i in range(pair):
            copies.append(
                pltpu.make_async_copy(
                    part.at[i],
                    out.at[
                        pl.ds(i * BLK + row0, rows), pl.ds(pl.multiple_of(h * width, width), width)
                    ],
                    sems.at[g, i],
                )
            )
    for copy in copies:
        copy.start()
    for copy in copies:
        copy.wait()


def exchange(queries, keys, values, source_block, doc_of_block):
    shards = lax.axis_size("ctx")
    groups = lax.axis_size("head")
    me = lax.axis_index("ctx")
    spot = jnp.stack([me, lax.axis_index("head")])
    row_count, width = queries.shape
    blocks = row_count // BLK
    pair = blocks // groups
    dtype = queries.dtype
    pack_position = jnp.arange(shards * blocks, dtype=jnp.int32)
    held = me * blocks + jnp.arange(blocks, dtype=jnp.int32)
    position = jnp.sum(
        jnp.where(source_block[None, :] == held[:, None], pack_position[None, :], 0), axis=1
    )
    dest = position // blocks

    kv_out = pl.pallas_call(
        pack_kv_out,
        out_shape=jax.ShapeDtypeStruct((shards, BLK, 2 * HEAD_SIZE), dtype),
        in_specs=[SMEM, VMEM, VMEM],
        out_specs=HBM,
        scratch_shapes=[pltpu.SemaphoreType.DMA((2, blocks))],
        name="pack_kv_out",
    )(dest, keys.reshape(blocks, BLK, HEAD_SIZE), values.reshape(blocks, BLK, HEAD_SIZE))
    kv_got = lax.all_to_all(kv_out, "ctx", split_axis=0, concat_axis=0, tiled=True)

    query_blocks = queries.reshape(blocks, BLK, width)
    q_out = pl.pallas_call(
        pack_queries,
        out_shape=[jax.ShapeDtypeStruct((shards, rows, width), dtype) for rows in ROWS],
        grid_spec=pltpu.PrefetchScalarGridSpec(
            num_scalar_prefetch=1,
            grid=(blocks,),
            in_specs=[pl.BlockSpec((1, BLK, width), lambda b, dest: (b, 0, 0))],
            out_specs=[
                pl.BlockSpec((1, rows, width), lambda b, dest: (dest[b], 0, 0)) for rows in ROWS
            ],
        ),
        name="pack_queries",
    )(dest, query_blocks)
    q_got = []
    for q in q_out:
        q_got.append(lax.all_to_all(q, "ctx", split_axis=0, concat_axis=0, tiled=True))

    owner = lax.dynamic_slice_in_dim(source_block, me * blocks, blocks) // blocks
    doc_ext = jnp.concatenate([jnp.full((REACH,), -1, jnp.int32), doc_of_block])
    docs = lax.dynamic_slice_in_dim(doc_ext, me * blocks, blocks + REACH)
    count = sum(
        (docs[REACH - d : REACH - d + blocks] == docs[REACH:]).astype(jnp.int32)
        for d in range(DOCMAX)
    )
    at = jnp.arange(blocks, dtype=jnp.int32)
    key = count * blocks + at
    rank = jnp.sum((key[None, :] < key[:, None]).astype(jnp.int32), axis=1)
    turn = jnp.sum(jnp.where(rank[None, :] == at[:, None], at[None, :], 0), axis=1)

    packed = pl.pallas_call(
        pack_kv_in,
        out_shape=jax.ShapeDtypeStruct((blocks, BLK, 2 * HEAD_SIZE), dtype),
        in_specs=[SMEM, HBM],
        out_specs=VMEM,
        scratch_shapes=[pltpu.SemaphoreType.DMA((blocks,))],
        name="pack_kv_in",
    )(owner, kv_got)
    route = [(i, i + 1) for i in range(shards - 1)]
    halo = lax.ppermute(packed[blocks - REACH :], "ctx", route)

    result = None
    row0 = 0
    for r, (got, rows) in enumerate(zip(q_got, ROWS)):
        spread = r < len(ROWS) - 1
        step = groups // HALVES if spread else groups
        parts = [None] * groups
        for first in reversed(range(0, groups, step)):
            items = step * pair
            scratch = [
                pltpu.VMEM((items, rows, width), dtype),
                pltpu.VMEM(((blocks + REACH) * BLK, HEAD_SIZE), dtype),
                pltpu.VMEM(((blocks + REACH) * BLK, 2 * HEAD_SIZE), dtype),
                pltpu.SemaphoreType.DMA((items,)),
            ]
            if spread:
                shape = [jax.ShapeDtypeStruct((pair, rows, width), dtype)] * step
                scratch = [
                    pltpu.VMEM((items, rows, width), dtype),
                    pltpu.SemaphoreType.DMA((step,)),
                ] + scratch
            else:
                shape = jax.ShapeDtypeStruct((blocks, rows, width), dtype)
            attended = pl.pallas_call(
                functools.partial(attend, row0, GROUP[r], first if spread else None),
                out_shape=shape,
                in_specs=[SMEM] * 4 + [HBM, VMEM, VMEM],
                out_specs=[HBM] * step if spread else VMEM,
                scratch_shapes=scratch,
            )(spot, owner, count, turn, got, packed, halo)
            if spread:
                for k in range(first, first + step):
                    swap = [(i, i ^ k) for i in range(groups)]
                    part = attended[k - first]
                    parts[k] = lax.ppermute(part, "head", swap) if k else part
            else:
                parts = [
                    lax.all_to_all(
                        attended.reshape(groups, pair * rows, width),
                        "head",
                        split_axis=0,
                        concat_axis=0,
                        tiled=True,
                    ).reshape(groups, pair, rows, width)
                ]
        before = [] if result is None else [result]
        result = pl.pallas_call(
            functools.partial(place, row0, spread, bool(before)),
            out_shape=jax.ShapeDtypeStruct((pair * BLK, groups * width), dtype),
            in_specs=[SMEM] + [VMEM] * len(parts) + [HBM] * len(before),
            out_specs=HBM,
            scratch_shapes=[pltpu.SemaphoreType.DMA((groups, pair))],
            input_output_aliases={1 + len(parts): 0} if before else {},
        )(spot, *parts, *before)
        row0 += rows
    return result


def solution(mesh):
    in_specs = (P("ctx", "head"), P("ctx", "head"), P("ctx", "head"), P(), P())
    out_specs = P(("ctx", "head"), None)
    return jax.shard_map(exchange, mesh=mesh, in_specs=in_specs, out_specs=out_specs, check_vma=False)
```
